128 devices in a mesh: blk: 32 (over z, y, core), rep: 4 (over x).
Axes of the slice: x: 4, y: 4, z: 4, core: 2. Of those that a mesh axis runs over, the one named last changes fastest.
Arguments:
- source_blocks: bfloat16 [256, 1024, 1024], P('blk', 'rep'), may hold values from -6 to 6
- coefficients: float32 [256, 2], P('blk'), may hold values from 0.3 to 1
- target_sector: int32 [256, 2], P('blk'), may hold values from 0 to 127, as said below
Outputs:
- recoupled: bfloat16 [128, 1024, 1024], P('blk', 'rep')
- density: float32 [128, 1024, 1024], P('blk', None, 'rep')
The draws below stay inside these ranges and needn't reach their ends.
Inputs may be any that keep to these rules, and one draw needn't show every extreme that they name: `target_sector`: sector t is owned by index t // 4 of blk. The 16 entries of one index of blk name sectors of any one owner at most 1 times, counted with repeats; one owner, the same for all indices, is named exactly 1 times by each index. A row never names one sector twice.
All inputs are finite; a program needn't handle non-finite values.
Results may differ from the reference program's by a relative error of at most 0.009.
Values may be sent and summed in bfloat16 or wider, within the bound.
A program may use at most 320 MiB of HBM per device.

```python
import jax
import jax.numpy as jnp
from jax import lax

BR = 1024
BC = 1024
TOP = 2
SRC_DEV = 8
TGT_DEV = 4
SOURCES = 256
SECTORS = 128
CAP = 1


def draw_target_sector(key, part):
    groups = SOURCES // SRC_DEV
    slot_total = groups * CAP
    entries = SRC_DEV * TOP
    key_full, key_rows = jax.random.split(jax.random.fold_in(key, 71))
    full_owner = jax.random.randint(key_full, (), 0, groups)

    def device_targets(subkey):
        key_one, key_two, key_three = jax.random.split(subkey, 3)
        slot_ids = (jnp.arange(slot_total, dtype=jnp.int32) + full_owner * CAP) % slot_total
        remainder = slot_ids[CAP:][jax.random.permutation(key_one, slot_total - CAP)]
        chosen = jnp.concatenate([slot_ids[:CAP], remainder])[:entries]
        chosen = chosen[jax.random.permutation(key_two, entries)]
        owners = chosen // CAP
        within = jax.random.randint(key_three, (entries,), 0, TGT_DEV)
        return (owners * TGT_DEV + within).astype(jnp.int32).reshape(SRC_DEV, TOP)
    subkeys = jax.random.split(key_rows, groups)
    return jax.vmap(device_targets)(subkeys).reshape(SOURCES, TOP)


def block_levels(stream_key, shape, pieces, least, top_value):
    loudness, own = 1.0, jax.random.fold_in(stream_key, 6)
    for dim, shards_of in pieces:
        steps = jnp.exp(jax.random.uniform(jax.random.fold_in(own, dim), (shards_of,), jnp.float32, least / len(pieces), top_value / len(pieces)))
        loudness = loudness * jnp.repeat(steps, shape[dim] // shards_of).reshape([-1 if axis == dim else 1 for axis in range(len(shape))])
    return loudness


def centred(key, extent, width, most, cuts=(), kind=jnp.bfloat16):
    loudness = block_levels(key, extent, cuts, -0.22, 0.18) if cuts else 1.0
    values = jax.random.normal(key, extent, jnp.float32) * width * loudness
    return jnp.minimum(jnp.maximum(values, -most), most).astype(kind)


def setup_inputs(seed: int = 0) -> dict:
    streams_of = jax.random.split(jax.random.key(seed), 4)
    source_blocks = centred(streams_of[0], (SOURCES, BR, BC), 1.0, 6.0, ((0, 32), (1, 4)))
    coefficients = jnp.clip(0.3 + 0.7 * jax.random.uniform(streams_of[1], (SOURCES, TOP), jnp.float32) ** block_levels(streams_of[1], (SOURCES, TOP), ((0, 32),), -0.2, 0.2), 0.3, 1.0)
    target_sector = draw_target_sector(jax.random.fold_in(streams_of[3], 71), 0)
    return dict(source_blocks=source_blocks, coefficients=coefficients, target_sector=target_sector)


def reference(source_blocks, coefficients, target_sector):
    height = source_blocks.shape[1]
    breadth = source_blocks.shape[2]
    accum = jnp.zeros((SECTORS, height, breadth), jnp.float32)

    def update(running, entry):
        source_id = (entry // TOP).astype(jnp.int32)
        column_id = (entry % TOP).astype(jnp.int32)
        source = lax.dynamic_index_in_dim(source_blocks, source_id, 0, keepdims=False)
        weight = coefficients[source_id, column_id]
        sector = target_sector[source_id, column_id].astype(jnp.int32)
        scaled = (weight * source.astype(jnp.float32)).astype(jnp.bfloat16)
        scaled = lax.optimization_barrier(scaled).astype(jnp.float32)
        current = lax.dynamic_index_in_dim(running, sector, 0, keepdims=False)
        running = lax.dynamic_update_index_in_dim(running, current + scaled, sector, 0)
        return running, None

    accum, unused = lax.scan(update, accum, jnp.arange(SOURCES * TOP, dtype=jnp.int32))
    recoupled = accum.astype(jnp.bfloat16)

    def single_gram(single):
        return jnp.dot(single.T, single, preferred_element_type=jnp.float32)

    density = lax.map(single_gram, recoupled)
    return recoupled, density
```

```python
import functools

import jax
import jax.numpy as jnp
from jax import lax
from jax.experimental import pallas as pl
from jax.experimental.pallas import tpu as pltpu
from jax.sharding import PartitionSpec as P

MESH = pl.DeviceIdType.MESH
BF = jnp.bfloat16
F32 = jnp.float32

ROWS = 16
CW = 256
HALF = 128
HCOL = 512
NCC = HCOL // CW
NCH = (HALF // ROWS) * NCC
L_A2, L_CB, L_R2, L_FN, L_X2 = 2, 4, 6, 8, 10
STEPS = NCH + L_X2
OFFS = (0, 1, 3, 2)


def kernel(src, tbl, rec_out, den_out, G, TB, W, PS, T, F, Q, RG, D,
           s_in, s_a1, s_a2, s_r1, s_r2, s_d, s_x1, s_x2, s_t,
           n_in, n_a1, n_a2, n_r1, n_r2, n_d, n_x1, n_x2, n_t, s_out):
    blk = lax.axis_index("blk")
    x = lax.axis_index("rep")
    z = blk // 8
    y = (blk // 2) % 4
    c = blk % 2
    oc = 1 - c

    def at_z(k, core):
        return ((((z + k) % 4) * 4 + y) * 2 + core, x)

    def at_y(k, core):
        return ((z * 4 + (y + k) % 4) * 2 + core, x)

    def at_x(k, core):
        return ((z * 4 + y) * 2 + core, (x + k) % 4)

    partner = (blk + 1 - 2 * c, x)
    gather_at = (at_z, at_y)
    scatter_at = (at_y, at_z)

    def rcopy(a, b, ssem, rsem, dev):
        pltpu.make_async_remote_copy(
            src_ref=a, dst_ref=b, send_sem=ssem, recv_sem=rsem,
            device_id=dev, device_id_type=MESH).start()

    def waiter(ref, ssem, rsem):
        return pltpu.make_async_remote_copy(
            src_ref=ref, dst_ref=ref, send_sem=ssem, recv_sem=rsem,
            device_id=partner, device_id_type=MESH)

    def got(ref, sem):
        waiter(ref, n_d.at[0], sem).wait_recv()

    def sent(ref, sem):
        waiter(ref, sem, s_d.at[0]).wait_send()

    peers = [partner]
    for k in (1, 2, 3):
        for core in (0, 1):
            peers.append(at_z(k, core))
            peers.append(at_y(k, core))
    for k in (1, 3):
        for core in (0, 1):
            peers.append(at_x(k, core))
    barrier = pltpu.get_barrier_semaphore()
    for dev in peers:
        pl.semaphore_signal(barrier, inc=1, device_id=dev, device_id_type=MESH)
    pl.semaphore_wait(barrier, len(peers))

    def place(q):
        rc = q // NCC
        cc = q % NCC
        r0 = pl.multiple_of(rc * ROWS, ROWS)
        c0 = pl.multiple_of(cc * CW, CW)
        return r0, c0, pl.ds(r0, ROWS), pl.ds(c0, CW)

    for p in range(2):
        rcopy(tbl, TB.at[p, 0, c], n_t.at[0], s_t.at[0], partner)
        for slot in (1, 2, 3):
            for core in (0, 1):
                rcopy(tbl, TB.at[p, slot, c], n_t.at[1], s_t.at[1],
                      gather_at[p](OFFS[slot], core))

    def load(q, carry):
        r0, c0, rows, cols = place(q)
        for p in range(2):
            cs = pl.ds(pl.multiple_of(p * HCOL + c0, CW), CW)
            mine = src.at[:, pl.ds(pl.multiple_of(c * HALF + r0, ROWS), ROWS), cs]
            other = src.at[:, pl.ds(pl.multiple_of(oc * HALF + r0, ROWS), ROWS), cs]
            dst = G.at[p, 0, pl.ds(c * 8, 8), rows, cols]
            pltpu.make_async_copy(mine, dst, s_in.at[q]).start()
            rcopy(other, dst, n_in.at[0], s_in.at[q], partner)
        return carry

    lax.fori_loop(0, NCH, load, 0)

    def stage_a1(q):
        _, _, rows, cols = place(q)
        got(G.at[:, 0, :, rows, cols], s_in.at[q])
        for p in range(2):
            mine = G.at[p, 0, :, rows, cols]
            rcopy(mine, G.at[p, 1, :, rows, cols], n_a1.at[0], s_a1.at[q], gather_at[p](1, c))
            rcopy(mine, G.at[p, 2, :, rows, cols], n_a1.at[1], s_a1.at[q], gather_at[p](3, c))

    def stage_a2(q):
        _, _, rows, cols = place(q)
        got(G.at[:, 1:3, :, rows, cols], s_a1.at[q])
        for p in range(2):
            rcopy(G.at[p, 1, 0:8, rows, cols], G.at[p, 3, 0:8, rows, cols],
                  n_a2.at[0], s_a2.at[q], gather_at[p](1, c))
            rcopy(G.at[p, 2, 8:16, rows, cols], G.at[p, 3, 8:16, rows, cols],
                  n_a2.at[1], s_a2.at[q], gather_at[p](3, c))

    def stage_cb(q):
        _, _, rows, cols = place(q)
        got(G.at[:, 3, :, rows, cols], s_a2.at[q])
        for p in range(2):
            s = G[p, :, :, rows, cols].reshape(64 * ROWS, CW)
            o = jnp.dot(W[p], s, preferred_element_type=F32)
            PS[p, :, :, rows, cols] = o.reshape(4, 8, ROWS, CW).astype(BF)
        for p in range(2):
            rcopy(PS.at[p, 3, 0:4, rows, cols], T.at[p, 0, :, rows, cols],
                  n_r1.at[0], s_r1.at[q], scatter_at[p](1, c))
            rcopy(PS.at[p, 3, 4:8, rows, cols], T.at[p, 1, :, rows, cols],
                  n_r1.at[1], s_r1.at[q], scatter_at[p](3, c))

    def stage_r2(q):
        _, _, rows, cols = place(q)
        got(T.at[:, :, :, rows, cols], s_r1.at[q])
        for p in range(2):
            a = PS[p, 1, 0:4, rows, cols].astype(F32) + T[p, 0, :, rows, cols].astype(F32)
            PS[p, 1, 0:4, rows, cols] = a.astype(BF)
            b = PS[p, 2, 4:8, rows, cols].astype(F32) + T[p, 1, :, rows, cols].astype(F32)
            PS[p, 2, 4:8, rows, cols] = b.astype(BF)
        for p in range(2):
            rcopy(PS.at[p, 1, :, rows, cols], F.at[p, 0, :, rows, cols],
                  n_r2.at[0], s_r2.at[q], scatter_at[p](1, c))
            rcopy(PS.at[p, 2, :, rows, cols], F.at[p, 1, :, rows, cols],
                  n_r2.at[1], s_r2.at[q], scatter_at[p](3, c))

    def stage_fn(q):
        _, _, rows, cols = place(q)
        got(F.at[:, :, :, rows, cols], s_r2.at[q])
        for p in range(2):
            for which in (oc, c):
                ks = pl.ds(which * 4, 4)
                v = (PS[p, 0, ks, rows, cols].astype(F32)
                     + F[p, 0, ks, rows, cols].astype(F32)
                     + F[p, 1, ks, rows, cols].astype(F32)).astype(BF)
                if which is c:
                    RG[0, :, c, p, rows, cols] = v
                else:
                    Q[:, p, rows, cols] = v
        away = Q.at[:, :, rows, cols]
        kept = RG.at[0, :, c, :, rows, cols]
        for slot, k in ((1, 1), (2, 3)):
            dst = RG.at[slot, :, c, :, rows, cols]
            rcopy(away, dst, n_x1.at[slot - 1], s_x1.at[q], at_x(k, oc))
            rcopy(kept, dst, n_x1.at[slot - 1], s_x1.at[q], at_x(k, c))
        rcopy(away, kept, n_d.at[0], s_d.at[q], partner)

    def stage_x2(q):
        _, _, rows, cols = place(q)
        got(RG.at[1:3, :, :, :, rows, cols], s_x1.at[q])
        rcopy(RG.at[1, :, 0, :, rows, cols], RG.at[3, :, 0, :, rows, cols],
              n_x2.at[0], s_x2.at[q], at_x(1, c))
        rcopy(RG.at[2, :, 1, :, rows, cols], RG.at[3, :, 1, :, rows, cols],
              n_x2.at[1], s_x2.at[q], at_x(3, c))

    def run(stage, q):
        @pl.when((q >= 0) & (q < NCH))
        def _():
            stage(q)

    stage_a1(0)
    stage_a1(1)

    got(TB.at[:, 0, 0], s_t.at[0])
    got(TB.at[:, 1:4], s_t.at[1])
    for p in range(2):
        TB[p, 0, c] = tbl[...]
    row = lax.broadcasted_iota(jnp.int32, (128, 128), 0)
    lane = lax.broadcasted_iota(jnp.int32, (128, 128), 1)
    same = (row % ROWS) == (lane % ROWS)
    sect = row // ROWS
    for p in range(2):
        for d in range(4):
            if p == 0:
                base = (z * 4 + (y + OFFS[d]) % 4) * 8
            else:
                base = (((z + OFFS[d]) % 4) * 4 + y) * 8
            want = (sect + base).astype(F32)

            def build(jk, carry, p=p, d=d, want=want):
                tab = TB[p, jk // 2, jk % 2]
                w = jnp.where(same & (tab[0:1, :] == want), tab[2:3, :], 0.0)
                w = w + jnp.where(same & (tab[1:2, :] == want), tab[3:4, :], 0.0)
                W[p, d * 128:(d + 1) * 128, pl.ds(pl.multiple_of(jk * 128, 128), 128)] = w.astype(BF)
                return carry

            lax.fori_loop(0, 8, build, 0)

    def step(s, carry):
        run(stage_a1, s + 2)
        run(stage_a2, s + 2 - L_A2)
        run(stage_x2, s + 2 - L_X2)
        run(stage_fn, s + 2 - L_FN)
        run(stage_r2, s + 2 - L_R2)
        run(stage_cb, s + 2 - L_CB)
        return carry

    lax.fori_loop(0, STEPS - 2, step, 0)

    def last_d(q, carry):
        _, _, rows, cols = place(q)
        got(RG.at[0, :, oc, :, rows, cols], s_d.at[q])
        return carry

    lax.fori_loop(0, NCH, last_d, 0)
    outs = []
    for h in range(2):
        for p in range(2):
            cp = pltpu.make_async_copy(
                RG.at[0, :, h, p],
                rec_out.at[:, h * HALF:(h + 1) * HALF, p * HCOL:(p + 1) * HCOL],
                s_out.at[h * 2 + p])
            cp.start()
            outs.append(cp)

    def last_x(q, carry):
        _, _, rows, cols = place(q)
        got(RG.at[3, :, :, :, rows, cols], s_x2.at[q])
        return carry

    lax.fori_loop(0, NCH, last_x, 0)

    xp = x // 2
    xo = pl.multiple_of((x % 2) * 256, 256)

    def gram(w, carry):
        rhs = RG[:, w, :, xp, :, pl.ds(xo, 256)].reshape(1024, 256)
        for p in range(2):
            lhs = RG[:, w, :, p].reshape(1024, HCOL)
            D[w, p * HCOL:(p + 1) * HCOL, :] = lax.dot_general(
                lhs, rhs, (((0,), (0,)), ((), ())), preferred_element_type=F32)
        pltpu.make_async_copy(D.at[w], den_out.at[w], s_out.at[4 + w]).start()
        return carry

    lax.fori_loop(0, 4, gram, 0)

    for w in range(4):
        pltpu.make_async_copy(D.at[w], den_out.at[w], s_out.at[4 + w]).wait()
    for cp in outs:
        cp.wait()

    sent(TB.at[:, 0, 0], n_t.at[0])
    sent(TB.at[:, 1:4], n_t.at[1])
    sent(src.at[:, 0:HALF, :], n_in.at[0])
    for k in range(2):
        sent(G.at[:, 0], n_a1.at[k])
        sent(G.at[:, 3, 0:8], n_a2.at[k])
        sent(T.at[:, 0], n_r1.at[k])
        sent(F.at[:, 0], n_r2.at[k])
        sent(RG.at[1], n_x1.at[k])
        sent(Q, n_x2.at[k])
    sent(Q, n_d.at[0])


def body(source_blocks, coefficients, target_sector):
    tab = jnp.concatenate([target_sector.T.astype(F32), coefficients.T], axis=0)
    tab = jnp.pad(jnp.repeat(tab, ROWS, axis=1), ((0, 4), (0, 0)))
    dma = pltpu.SemaphoreType.DMA
    chunk_sems = [dma((NCH,)) for _ in range(8)]
    return pl.pallas_call(
        kernel,
        out_shape=(jax.ShapeDtypeStruct((4, 256, 1024), BF),
                   jax.ShapeDtypeStruct((4, 1024, 256), F32)),
        in_specs=[pl.BlockSpec(memory_space=pl.ANY),
                  pl.BlockSpec(memory_space=pltpu.VMEM)],
        out_specs=(pl.BlockSpec(memory_space=pl.ANY),
                   pl.BlockSpec(memory_space=pl.ANY)),
        scratch_shapes=[
            pltpu.VMEM((2, 4, 16, HALF, HCOL), BF),
            pltpu.VMEM((2, 4, 2, 8, 128), F32),
            pltpu.VMEM((2, 512, 1024), BF),
            pltpu.VMEM((2, 4, 8, HALF, HCOL), BF),
            pltpu.VMEM((2, 2, 4, HALF, HCOL), BF),
            pltpu.VMEM((2, 2, 8, HALF, HCOL), BF),
            pltpu.VMEM((4, 2, HALF, HCOL), BF),
            pltpu.VMEM((4, 4, 2, 2, HALF, HCOL), BF),
            pltpu.VMEM((4, 1024, 256), F32),
            *chunk_sems,
            dma((2,)),
            dma((1,)), dma((2,)), dma((2,)), dma((2,)), dma((2,)), dma((1,)),
            dma((2,)), dma((2,)), dma((2,)),
            dma((8,)),
        ],
        compiler_params=pltpu.CompilerParams(
            collective_id=0, has_side_effects=True, vmem_limit_bytes=64 * 1024 * 1024 - 65536),
        name="recouple",
    )(source_blocks, tab)


def solution(mesh):
    in_specs = (P("blk", "rep", None), P("blk", None), P("blk", None))
    out_specs = (P("blk", "rep", None), P("blk", None, "rep"))
    return jax.shard_map(body, mesh=mesh, in_specs=in_specs, out_specs=out_specs, check_vma=False)
```

```python
import functools

import jax
import jax.numpy as jnp
from jax import lax
from jax.experimental import pallas as pl
from jax.experimental.pallas import tpu as pltpu
from jax.sharding import PartitionSpec as P

MESH = pl.DeviceIdType.MESH
BF = jnp.bfloat16
F32 = jnp.float32

ROWS = 16
CW = 128
HALF = 128
HCOL = 512
NCC = HCOL // CW
NCH = (HALF // ROWS) * NCC
LOOK = 2
L_CB, L_R2, L_FN, L_X2 = 2, 4, 6, 8
STEPS = NCH + L_X2
OFFS = (0, 1, 3, 2)


def kernel(src, coef, targ, RG, G, MT, TB, W, PS, T, F, Q,
           s_in, s_a1, s_a2, s_r1, s_r2, s_d, s_x1, s_x2, s_t,
           n_in, n_a1, n_a2, n_r1, n_r2, n_d, n_x1, n_x2, n_t):
    blk = lax.axis_index("blk")
    x = lax.axis_index("rep")
    z = blk // 8
    y = (blk // 2) % 4
    c = blk % 2
    oc = 1 - c

    def at_z(k, core):
        return ((((z + k) % 4) * 4 + y) * 2 + core, x)

    def at_y(k, core):
        return ((z * 4 + (y + k) % 4) * 2 + core, x)

    def at_x(k, core):
        return ((z * 4 + y) * 2 + core, (x + k) % 4)

    partner = (blk + 1 - 2 * c, x)
    gather_at = (at_z, at_y)
    scatter_at = (at_y, at_z)

    def rcopy(a, b, ssem, rsem, dev):
        pltpu.make_async_remote_copy(
            src_ref=a, dst_ref=b, send_sem=ssem, recv_sem=rsem,
            device_id=dev, device_id_type=MESH).start()

    def waiter(ref, ssem, rsem):
        return pltpu.make_async_remote_copy(
            src_ref=ref, dst_ref=ref, send_sem=ssem, recv_sem=rsem,
            device_id=partner, device_id_type=MESH)

    def got(ref, sem):
        waiter(ref, n_d.at[0], sem).wait_recv()

    def sent(ref, sem):
        waiter(ref, sem, s_d.at[0]).wait_send()

    trow = lax.broadcasted_iota(jnp.int32, (8, 128), 0)
    tblk = lax.broadcasted_iota(jnp.int32, (8, 128), 1) // ROWS
    mt = jnp.zeros((8, 128), F32)
    for k in range(2):
        for b in range(8):
            mt = jnp.where((trow == k) & (tblk == b), targ[k, b].astype(F32), mt)
            mt = jnp.where((trow == k + 2) & (tblk == b), coef[k, b], mt)
    MT[...] = mt

    peers = [partner]
    for k in (1, 2, 3):
        for core in (0, 1):
            peers.append(at_z(k, core))
            peers.append(at_y(k, core))
    for k in (1, 3):
        for core in (0, 1):
            peers.append(at_x(k, core))
    barrier = pltpu.get_barrier_semaphore()
    for dev in peers:
        pl.semaphore_signal(barrier, inc=1, device_id=dev, device_id_type=MESH)
    pl.semaphore_wait(barrier, len(peers))

    def place(q):
        rc = q // NCC
        cc = q % NCC
        r0 = pl.multiple_of(rc * ROWS, ROWS)
        c0 = pl.multiple_of(cc * CW, CW)
        return r0, c0, pl.ds(r0, ROWS), pl.ds(c0, CW)

    def load(q):
        r0, c0, rows, cols = place(q)
        for p in range(2):
            cs = pl.ds(pl.multiple_of(p * HCOL + c0, CW), CW)
            mine = src.at[:, pl.ds(pl.multiple_of(c * HALF + r0, ROWS), ROWS), cs]
            other = src.at[:, pl.ds(pl.multiple_of(oc * HALF + r0, ROWS), ROWS), cs]
            dst = G.at[p, 0, pl.ds(c * 8, 8), rows, cols]
            pltpu.make_async_copy(mine, dst, s_in.at[q]).start()
            rcopy(other, dst, n_in.at[0], s_in.at[q], partner)

    def stage_a1(q):
        r0, c0, rows, cols = place(q)
        own = pl.ds(c * 8, 8)
        for p in range(2):
            cs = pl.ds(pl.multiple_of(p * HCOL + c0, CW), CW)
            for h in range(2):
                part = src.at[:, pl.ds(pl.multiple_of(h * HALF + r0, ROWS), ROWS), cs]
                rcopy(part, G.at[p, 1, own, rows, cols], n_a1.at[0], s_a1.at[q], gather_at[p](1, h))
                rcopy(part, G.at[p, 2, own, rows, cols], n_a1.at[1], s_a1.at[q], gather_at[p](3, h))

    def stage_a2(q):
        _, _, rows, cols = place(q)
        got(G.at[:, 1:3, :, rows, cols], s_a1.at[q])
        for p in range(2):
            rcopy(G.at[p, 1, 0:8, rows, cols], G.at[p, 3, 0:8, rows, cols],
                  n_a2.at[0], s_a2.at[q], gather_at[p](1, c))
            rcopy(G.at[p, 2, 8:16, rows, cols], G.at[p, 3, 8:16, rows, cols],
                  n_a2.at[1], s_a2.at[q], gather_at[p](3, c))

    def stage_cb(q):
        _, _, rows, cols = place(q)
        got(G.at[:, 0, :, rows, cols], s_in.at[q])
        got(G.at[:, 3, :, rows, cols], s_a2.at[q])
        for p in range(2):
            s = G[p, :, :, rows, cols].reshape(64 * ROWS, CW)
            o = jnp.dot(W[p], s, preferred_element_type=F32)
            PS[p, :, :, rows, cols] = o.reshape(4, 8, ROWS, CW).astype(BF)
        for p in range(2):
            rcopy(PS.at[p, 3, 0:4, rows, cols], T.at[p, 0, :, rows, cols],
                  n_r1.at[0], s_r1.at[q], scatter_at[p](1, c))
            rcopy(PS.at[p, 3, 4:8, rows, cols], T.at[p, 1, :, rows, cols],
                  n_r1.at[1], s_r1.at[q], scatter_at[p](3, c))

    def stage_r2(q):
        _, _, rows, cols = place(q)
        got(T.at[:, :, :, rows, cols], s_r1.at[q])
        for p in range(2):
            a = PS[p, 1, 0:4, rows, cols].astype(F32) + T[p, 0, :, rows, cols].astype(F32)
            PS[p, 1, 0:4, rows, cols] = a.astype(BF)
            b = PS[p, 2, 4:8, rows, cols].astype(F32) + T[p, 1, :, rows, cols].astype(F32)
            PS[p, 2, 4:8, rows, cols] = b.astype(BF)
        for p in range(2):
            rcopy(PS.at[p, 1, :, rows, cols], F.at[p, 0, :, rows, cols],
                  n_r2.at[0], s_r2.at[q], scatter_at[p](1, c))
            rcopy(PS.at[p, 2, :, rows, cols], F.at[p, 1, :, rows, cols],
                  n_r2.at[1], s_r2.at[q], scatter_at[p](3, c))

    def stage_fn(q):
        _, _, rows, cols = place(q)
        got(F.at[:, :, :, rows, cols], s_r2.at[q])
        for p in range(2):
            for which in (oc, c):
                ks = pl.ds(which * 4, 4)
                v = (PS[p, 0, ks, rows, cols].astype(F32)
                     + F[p, 0, ks, rows, cols].astype(F32)
                     + F[p, 1, ks, rows, cols].astype(F32)).astype(BF)
                if which is c:
                    RG[0, :, c, p, rows, cols] = v
                else:
                    Q[:, p, rows, cols] = v
        away = Q.at[:, :, rows, cols]
        kept = RG.at[0, :, c, :, rows, cols]
        for slot, k in ((1, 1), (2, 3)):
            dst = RG.at[slot, :, c, :, rows, cols]
            rcopy(away, dst, n_x1.at[slot - 1], s_x1.at[q], at_x(k, oc))
            rcopy(kept, dst, n_x1.at[slot - 1], s_x1.at[q], at_x(k, c))
        rcopy(away, kept, n_d.at[0], s_d.at[q], partner)

    def stage_x2(q):
        _, _, rows, cols = place(q)
        got(RG.at[1:3, :, :, :, rows, cols], s_x1.at[q])
        rcopy(RG.at[1, :, 0, :, rows, cols], RG.at[3, :, 0, :, rows, cols],
              n_x2.at[0], s_x2.at[q], at_x(1, c))
        rcopy(RG.at[2, :, 1, :, rows, cols], RG.at[3, :, 1, :, rows, cols],
              n_x2.at[1], s_x2.at[q], at_x(3, c))

    def run(stage, q):
        @pl.when((q >= 0) & (q < NCH))
        def _():
            stage(q)

    for q in range(LOOK):
        stage_a1(q)
    for p in range(2):
        rcopy(MT, TB.at[p, 0, c], n_t.at[0], s_t.at[0], partner)
        for slot in (1, 2, 3):
            for core in (0, 1):
                rcopy(MT, TB.at[p, slot, c], n_t.at[1], s_t.at[1],
                      gather_at[p](OFFS[slot], core))
    for q in range(LOOK):
        load(q)

    got(TB.at[:, 0, 0], s_t.at[0])
    got(TB.at[:, 1:4], s_t.at[1])
    for p in range(2):
        TB[p, 0, c] = mt
    row = lax.broadcasted_iota(jnp.int32, (128, 128), 0)
    lane = lax.broadcasted_iota(jnp.int32, (128, 128), 1)
    same = (row % ROWS) == (lane % ROWS)
    sect = row // ROWS
    for p in range(2):
        for d in range(4):
            if p == 0:
                base = (z * 4 + (y + OFFS[d]) % 4) * 8
            else:
                base = (((z + OFFS[d]) % 4) * 4 + y) * 8
            want = (sect + base).astype(F32)

            def build(jk, carry, p=p, d=d, want=want):
                tab = TB[p, jk // 2, jk % 2]
                w = jnp.where(same & (tab[0:1, :] == want), tab[2:3, :], 0.0)
                w = w + jnp.where(same & (tab[1:2, :] == want), tab[3:4, :], 0.0)
                W[p, d * 128:(d + 1) * 128, pl.ds(pl.multiple_of(jk * 128, 128), 128)] = w.astype(BF)
                return carry

            lax.fori_loop(0, 8, build, 0)

    def step(s, carry):
        run(stage_x2, s - L_X2)
        run(stage_fn, s - L_FN)
        run(stage_r2, s - L_R2)
        run(stage_cb, s - L_CB)
        run(stage_a2, s)
        run(stage_a1, s + LOOK)
        run(load, s + LOOK)
        return carry

    lax.fori_loop(0, STEPS, step, 0)

    def last(q, carry):
        _, _, rows, cols = place(q)
        got(RG.at[0, :, oc, :, rows, cols], s_d.at[q])
        got(RG.at[3, :, :, :, rows, cols], s_x2.at[q])
        return carry

    lax.fori_loop(0, NCH, last, 0)

    sent(TB.at[:, 0, 0], n_t.at[0])
    sent(TB.at[:, 1:4], n_t.at[1])
    sent(src.at[:, 0:HALF, :], n_in.at[0])
    for k in range(2):
        sent(G.at[:, 0], n_a1.at[k])
        sent(G.at[:, 3, 0:8], n_a2.at[k])
        sent(T.at[:, 0], n_r1.at[k])
        sent(F.at[:, 0], n_r2.at[k])
        sent(RG.at[1], n_x1.at[k])
        sent(Q, n_x2.at[k])
    sent(Q, n_d.at[0])


def finish(RG, rec_out, den_out, D, s_out):
    x = lax.axis_index("rep")
    outs = []
    for h in range(2):
        for p in range(2):
            cp = pltpu.make_async_copy(
                RG.at[0, :, h, p],
                rec_out.at[:, h * HALF:(h + 1) * HALF, p * HCOL:(p + 1) * HCOL],
                s_out.at[h * 2 + p])
            cp.start()
            outs.append(cp)
    xp = x // 2
    xo = pl.multiple_of((x % 2) * 256, 256)

    def gram(w, carry):
        rhs = RG[:, w, :, xp, :, pl.ds(xo, 256)].reshape(1024, 256)
        for p in range(2):
            lhs = RG[:, w, :, p].reshape(1024, HCOL)
            D[w, p * HCOL:(p + 1) * HCOL, :] = lax.dot_general(
                lhs, rhs, (((0,), (0,)), ((), ())), preferred_element_type=F32)
        pltpu.make_async_copy(D.at[w], den_out.at[w], s_out.at[4 + w]).start()
        return carry

    lax.fori_loop(0, 4, gram, 0)
    for w in range(4):
        pltpu.make_async_copy(D.at[w], den_out.at[w], s_out.at[4 + w]).wait()
    for cp in outs:
        cp.wait()


def body(source_blocks, coefficients, target_sector):
    dma = pltpu.SemaphoreType.DMA
    chunk_sems = [dma((NCH,)) for _ in range(8)]
    gathered = pl.pallas_call(
        kernel,
        out_shape=pltpu.VMEM((4, 4, 2, 2, HALF, HCOL), BF),
        in_specs=[pl.BlockSpec(memory_space=pl.ANY),
                  pl.BlockSpec(memory_space=pltpu.SMEM),
                  pl.BlockSpec(memory_space=pltpu.SMEM)],
        out_specs=pl.BlockSpec(memory_space=pltpu.VMEM),
        scratch_shapes=[
            pltpu.VMEM((2, 4, 16, HALF, HCOL), BF),
            pltpu.VMEM((8, 128), F32),
            pltpu.VMEM((2, 4, 2, 8, 128), F32),
            pltpu.VMEM((2, 512, 1024), BF),
            pltpu.VMEM((2, 4, 8, HALF, HCOL), BF),
            pltpu.VMEM((2, 2, 4, HALF, HCOL), BF),
            pltpu.VMEM((2, 2, 8, HALF, HCOL), BF),
            pltpu.VMEM((4, 2, HALF, HCOL), BF),
            *chunk_sems,
            dma((2,)),
            dma((1,)), dma((2,)), dma((2,)), dma((2,)), dma((2,)), dma((1,)),
            dma((2,)), dma((2,)), dma((2,)),
        ],
        compiler_params=pltpu.CompilerParams(
            collective_id=0, has_side_effects=True, vmem_limit_bytes=50 * 1024 * 1024),
        name="recouple",
    )(source_blocks, coefficients.T, target_sector.T)
    return pl.pallas_call(
        finish,
        out_shape=(jax.ShapeDtypeStruct((4, 256, 1024), BF),
                   jax.ShapeDtypeStruct((4, 1024, 256), F32)),
        in_specs=[pl.BlockSpec(memory_space=pltpu.VMEM)],
        out_specs=(pl.BlockSpec(memory_space=pl.ANY),
                   pl.BlockSpec(memory_space=pl.ANY)),
        scratch_shapes=[pltpu.VMEM((4, 1024, 256), F32), dma((8,))],
        compiler_params=pltpu.CompilerParams(vmem_limit_bytes=24 * 1024 * 1024),
        name="finish",
    )(gathered)


def solution(mesh):
    in_specs = (P("blk", "rep", None), P("blk", None), P("blk", None))
    out_specs = (P("blk", "rep", None), P("blk", None, "rep"))
    return jax.shard_map(body, mesh=mesh, in_specs=in_specs, out_specs=out_specs, check_vma=False)
```

```python
import functools

import jax
import jax.numpy as jnp
from jax import lax
from jax.experimental import pallas as pl
from jax.experimental.pallas import tpu as pltpu
from jax.sharding import PartitionSpec as P

MESH = pl.DeviceIdType.MESH
BF = jnp.bfloat16
F32 = jnp.float32

ROWS = 16
CW = 128
HALF = 128
HCOL = 512
NCC = HCOL // CW
NCH = (HALF // ROWS) * NCC
A1, A2, PRE = 6, 2, 6
L_R2, L_FN, L_X2, L_X3 = 2, 4, 6, 8
STEPS = NCH + L_X3
KROWS = 32
GCH = (KROWS // ROWS) * NCC
KCON = 8 * KROWS
OFFS = (0, 1, 3, 2)


def kernel(src, coef_h, targ_h, RG, D, coef, targ, G, MT, TB, W, PS, T, F, Q,
           s_in, s_a1, s_a2, s_r1, s_r2, s_d, s_x1, s_x2, s_t,
           n_in, n_a1, n_a2, n_r1, n_r2, n_d, n_x1, n_x2, n_t, s_sm):
    blk = lax.axis_index("blk")
    x = lax.axis_index("rep")
    z = blk // 8
    y = (blk // 2) % 4
    c = blk % 2
    oc = 1 - c

    def at_z(k, core):
        return ((((z + k) % 4) * 4 + y) * 2 + core, x)

    def at_y(k, core):
        return ((z * 4 + (y + k) % 4) * 2 + core, x)

    def at_x(k, core):
        return ((z * 4 + y) * 2 + core, (x + k) % 4)

    partner = (blk + 1 - 2 * c, x)
    gather_at = (at_z, at_y)
    scatter_at = (at_y, at_z)

    def rcopy(a, b, ssem, rsem, dev):
        pltpu.make_async_remote_copy(
            src_ref=a, dst_ref=b, send_sem=ssem, recv_sem=rsem,
            device_id=dev, device_id_type=MESH).start()

    def waiter(ref, ssem, rsem):
        return pltpu.make_async_remote_copy(
            src_ref=ref, dst_ref=ref, send_sem=ssem, recv_sem=rsem,
            device_id=partner, device_id_type=MESH)

    def got(ref, sem):
        waiter(ref, n_d.at[0], sem).wait_recv()

    def sent(ref, sem):
        waiter(ref, sem, s_d.at[0]).wait_send()

    peers = [partner]
    for k in (1, 2, 3):
        for core in (0, 1):
            peers.append(at_z(k, core))
            peers.append(at_y(k, core))
    for k in (1, 3):
        for core in (0, 1):
            peers.append(at_x(k, core))
    barrier = pltpu.get_barrier_semaphore()
    for dev in peers:
        pl.semaphore_signal(barrier, inc=1, device_id=dev, device_id_type=MESH)
    small = [pltpu.make_async_copy(coef_h, coef, s_sm.at[0]),
             pltpu.make_async_copy(targ_h, targ, s_sm.at[1])]
    for cp in small:
        cp.start()
    for cp in small:
        cp.wait()

    trow = lax.broadcasted_iota(jnp.int32, (8, 128), 0)
    tblk = lax.broadcasted_iota(jnp.int32, (8, 128), 1) // ROWS
    mt = jnp.zeros((8, 128), F32)
    for k in range(2):
        for b in range(8):
            mt = jnp.where((trow == k) & (tblk == b), targ[k, b].astype(F32), mt)
            mt = jnp.where((trow == k + 2) & (tblk == b), coef[k, b], mt)
    MT[...] = mt

    pl.semaphore_wait(barrier, len(peers))

    def place(q):
        rc = q // NCC
        cc = q % NCC
        r0 = pl.multiple_of(rc * ROWS, ROWS)
        c0 = pl.multiple_of(cc * CW, CW)
        return r0, c0, pl.ds(r0, ROWS), pl.ds(c0, CW)

    def load(q):
        r0, c0, rows, cols = place(q)
        for p in range(2):
            cs = pl.ds(pl.multiple_of(p * HCOL + c0, CW), CW)
            mine = src.at[:, pl.ds(pl.multiple_of(c * HALF + r0, ROWS), ROWS), cs]
            other = src.at[:, pl.ds(pl.multiple_of(oc * HALF + r0, ROWS), ROWS), cs]
            dst = G.at[p, 0, pl.ds(c * 8, 8), rows, cols]
            pltpu.make_async_copy(mine, dst, s_in.at[q]).start()
            rcopy(other, dst, n_in.at[0], s_in.at[q], partner)

    def stage_a1(q):
        r0, c0, rows, cols = place(q)
        own = pl.ds(c * 8, 8)
        for p in range(2):
            cs = pl.ds(pl.multiple_of(p * HCOL + c0, CW), CW)
            for h in range(2):
                part = src.at[:, pl.ds(pl.multiple_of(h * HALF + r0, ROWS), ROWS), cs]
                rcopy(part, G.at[p, 1, own, rows, cols], n_a1.at[0], s_a1.at[q], gather_at[p](1, h))
                rcopy(part, G.at[p, 2, own, rows, cols], n_a1.at[1], s_a1.at[q], gather_at[p](3, h))

    def stage_a2(q):
        _, _, rows, cols = place(q)
        got(G.at[:, 1:3, :, rows, cols], s_a1.at[q])
        for p in range(2):
            rcopy(G.at[p, 1, 0:8, rows, cols], G.at[p, 3, 0:8, rows, cols],
                  n_a2.at[0], s_a2.at[q], gather_at[p](1, c))
            rcopy(G.at[p, 2, 8:16, rows, cols], G.at[p, 3, 8:16, rows, cols],
                  n_a2.at[1], s_a2.at[q], gather_at[p](3, c))

    def stage_cb(q):
        _, _, rows, cols = place(q)
        got(G.at[:, 0, :, rows, cols], s_in.at[q])
        got(G.at[:, 3, :, rows, cols], s_a2.at[q])
        for p in range(2):
            s = G[p, :, :, rows, cols].reshape(64 * ROWS, CW)
            o = jnp.dot(W[p], s, preferred_element_type=F32)
            PS[p, :, :, rows, cols] = o.reshape(4, 8, ROWS, CW).astype(BF)
        for p in range(2):
            rcopy(PS.at[p, 3, 0:4, rows, cols], T.at[p, 0, :, rows, cols],
                  n_r1.at[0], s_r1.at[q], scatter_at[p](1, c))
            rcopy(PS.at[p, 3, 4:8, rows, cols], T.at[p, 1, :, rows, cols],
                  n_r1.at[1], s_r1.at[q], scatter_at[p](3, c))

    def stage_r2(q):
        _, _, rows, cols = place(q)
        got(T.at[:, :, :, rows, cols], s_r1.at[q])
        for p in range(2):
            a = PS[p, 1, 0:4, rows, cols].astype(F32) + T[p, 0, :, rows, cols].astype(F32)
            PS[p, 1, 0:4, rows, cols] = a.astype(BF)
            b = PS[p, 2, 4:8, rows, cols].astype(F32) + T[p, 1, :, rows, cols].astype(F32)
            PS[p, 2, 4:8, rows, cols] = b.astype(BF)
        for p in range(2):
            rcopy(PS.at[p, 1, :, rows, cols], F.at[p, 0, :, rows, cols],
                  n_r2.at[0], s_r2.at[q], scatter_at[p](1, c))
            rcopy(PS.at[p, 2, :, rows, cols], F.at[p, 1, :, rows, cols],
                  n_r2.at[1], s_r2.at[q], scatter_at[p](3, c))

    def stage_fn(q):
        _, _, rows, cols = place(q)
        got(F.at[:, :, :, rows, cols], s_r2.at[q])
        for p in range(2):
            for which in (oc, c):
                ks = pl.ds(which * 4, 4)
                v = (PS[p, 0, ks, rows, cols].astype(F32)
                     + F[p, 0, ks, rows, cols].astype(F32)
                     + F[p, 1, ks, rows, cols].astype(F32)).astype(BF)
                if which is c:
                    RG[0, :, c, p, rows, cols] = v
                else:
                    Q[:, p, rows, cols] = v
        away = Q.at[:, :, rows, cols]
        kept = RG.at[0, :, c, :, rows, cols]
        for slot, k in ((1, 1), (2, 3)):
            dst = RG.at[slot, :, c, :, rows, cols]
            rcopy(away, dst, n_x1.at[slot - 1], s_x1.at[q], at_x(k, oc))
            rcopy(kept, dst, n_x1.at[slot - 1], s_x1.at[q], at_x(k, c))
        rcopy(away, kept, n_d.at[0], s_d.at[q], partner)

    def stage_x2(q):
        _, _, rows, cols = place(q)
        got(RG.at[1:3, :, :, :, rows, cols], s_x1.at[q])
        rcopy(RG.at[1, :, 0, :, rows, cols], RG.at[3, :, 0, :, rows, cols],
              n_x2.at[0], s_x2.at[q], at_x(1, c))
        rcopy(RG.at[2, :, 1, :, rows, cols], RG.at[3, :, 1, :, rows, cols],
              n_x2.at[1], s_x2.at[q], at_x(3, c))

    def stage_x3(q):
        _, _, rows, cols = place(q)
        got(RG.at[0, :, oc, :, rows, cols], s_d.at[q])
        got(RG.at[3, :, :, :, rows, cols], s_x2.at[q])

    xp = x // 2
    xo = pl.multiple_of((x % 2) * 256, 256)

    def gram(g, w):
        rows = pl.ds(pl.multiple_of(g * KROWS, KROWS), KROWS)
        rhs = RG[:, w, :, xp, rows, pl.ds(xo, 256)].reshape(KCON, 256)
        for p in range(2):
            lhs = RG[:, w, :, p, rows, :].reshape(KCON, HCOL)
            part = lax.dot_general(
                lhs, rhs, (((0,), (0,)), ((), ())), preferred_element_type=F32)
            at = slice(p * HCOL, (p + 1) * HCOL)

            @pl.when(g == 0)
            def _():
                D[w, at, :] = part

            @pl.when(g > 0)
            def _():
                D[w, at, :] += part

    def run(stage, q, least=0):
        @pl.when((q >= least) & (q < NCH))
        def _():
            stage(q)

    for p in range(2):
        rcopy(MT, TB.at[p, 0, c], n_t.at[0], s_t.at[0], partner)
        for slot in (1, 2, 3):
            for core in (0, 1):
                rcopy(MT, TB.at[p, slot, c], n_t.at[1], s_t.at[1],
                      gather_at[p](OFFS[slot], core))
    for q in range(PRE):
        stage_a1(q)
    for q in range(PRE):
        load(q)
    for q in range(A2):
        stage_a2(q)

    got(TB.at[:, 0, 0], s_t.at[0])
    got(TB.at[:, 1:4], s_t.at[1])
    for p in range(2):
        TB[p, 0, c] = mt
    row = lax.broadcasted_iota(jnp.int32, (128, 128), 0).astype(F32)
    lane = (lax.broadcasted_iota(jnp.int32, (1, 128), 1) % ROWS).astype(F32)
    for p in range(2):
        for d in range(4):
            if p == 0:
                base = (z * 4 + (y + OFFS[d]) % 4) * 8
            else:
                base = (((z + OFFS[d]) % 4) * 4 + y) * 8
            base = base.astype(F32)

            def build(jk, carry, p=p, d=d, base=base):
                tab = TB[p, jk // 2, jk % 2]
                i0 = (tab[0:1, :] - base) * ROWS + lane
                i1 = (tab[1:2, :] - base) * ROWS + lane
                w = jnp.where(row == i0, tab[2:3, :], jnp.where(row == i1, tab[3:4, :], 0.0))
                W[p, d * 128:(d + 1) * 128, pl.ds(pl.multiple_of(jk * 128, 128), 128)] = w.astype(BF)
                return carry

            lax.fori_loop(0, 8, build, 0)

    def step(s, carry):
        run(stage_a1, s + A1, PRE)
        run(stage_a2, s + A2)
        run(stage_cb, s)
        run(stage_r2, s - L_R2)
        run(stage_fn, s - L_FN)
        run(stage_x2, s - L_X2)
        run(stage_x3, s - L_X3)
        run(load, s + A1, PRE)
        piece = s - (GCH + L_X3)

        @pl.when((piece >= 0) & (piece % GCH < 4) & (piece // GCH < HALF // KROWS - 1))
        def _():
            gram(piece // GCH, piece % GCH)
        return carry

    lax.fori_loop(0, STEPS, step, 0)

    sent(TB.at[:, 0, 0], n_t.at[0])
    sent(TB.at[:, 1:4], n_t.at[1])
    sent(src.at[:, 0:HALF, :], n_in.at[0])
    for k in range(2):
        sent(G.at[:, 0], n_a1.at[k])
        sent(G.at[:, 3, 0:8], n_a2.at[k])
        sent(T.at[:, 0], n_r1.at[k])
        sent(F.at[:, 0], n_r2.at[k])
        sent(RG.at[1], n_x1.at[k])
        sent(Q, n_x2.at[k])
    sent(Q, n_d.at[0])


def finish(RG, D_in, rec_out, den_out, D, s_out):
    x = lax.axis_index("rep")
    outs = []
    for h in range(2):
        for p in range(2):
            cp = pltpu.make_async_copy(
                RG.at[0, :, h, p],
                rec_out.at[:, h * HALF:(h + 1) * HALF, p * HCOL:(p + 1) * HCOL],
                s_out.at[h * 2 + p])
            cp.start()
            outs.append(cp)
    xp = x // 2
    xo = pl.multiple_of((x % 2) * 256, 256)
    rows = slice(HALF - KROWS, HALF)

    def gram(w, carry):
        rhs = RG[:, w, :, xp, rows, pl.ds(xo, 256)].reshape(KCON, 256)
        for p in range(2):
            lhs = RG[:, w, :, p, rows, :].reshape(KCON, HCOL)
            at = slice(p * HCOL, (p + 1) * HCOL)
            D[w, at, :] = D_in[w, at, :] + lax.dot_general(
                lhs, rhs, (((0,), (0,)), ((), ())), preferred_element_type=F32)
        pltpu.make_async_copy(D.at[w], den_out.at[w], s_out.at[4 + w]).start()
        return carry

    lax.fori_loop(0, 4, gram, 0)
    for w in range(4):
        pltpu.make_async_copy(D.at[w], den_out.at[w], s_out.at[4 + w]).wait()
    for cp in outs:
        cp.wait()


def body(source_blocks, coefficients, target_sector):
    dma = pltpu.SemaphoreType.DMA
    chunk_sems = [dma((NCH,)) for _ in range(8)]
    gathered, partial = pl.pallas_call(
        kernel,
        out_shape=(pltpu.VMEM((4, 4, 2, 2, HALF, HCOL), BF),
                   pltpu.VMEM((4, 1024, 256), F32)),
        in_specs=[pl.BlockSpec(memory_space=pl.ANY),
                  pl.BlockSpec(memory_space=pl.ANY),
                  pl.BlockSpec(memory_space=pl.ANY)],
        out_specs=(pl.BlockSpec(memory_space=pltpu.VMEM),
                   pl.BlockSpec(memory_space=pltpu.VMEM)),
        scratch_shapes=[
            pltpu.SMEM((2, 8), F32),
            pltpu.SMEM((2, 8), jnp.int32),
            pltpu.VMEM((2, 4, 16, HALF, HCOL), BF),
            pltpu.VMEM((8, 128), F32),
            pltpu.VMEM((2, 4, 2, 8, 128), F32),
            pltpu.VMEM((2, 512, 1024), BF),
            pltpu.VMEM((2, 4, 8, HALF, HCOL), BF),
            pltpu.VMEM((2, 2, 4, HALF, HCOL), BF),
            pltpu.VMEM((2, 2, 8, HALF, HCOL), BF),
            pltpu.VMEM((4, 2, HALF, HCOL), BF),
            *chunk_sems,
            dma((2,)),
            dma((1,)), dma((2,)), dma((2,)), dma((2,)), dma((2,)), dma((1,)),
            dma((2,)), dma((2,)), dma((2,)),
            dma((2,)),
        ],
        compiler_params=pltpu.CompilerParams(
            collective_id=0, has_side_effects=True, vmem_limit_bytes=46 * 1024 * 1024),
        name="recouple",
    )(source_blocks, coefficients.T, target_sector.T)
    return pl.pallas_call(
        finish,
        out_shape=(jax.ShapeDtypeStruct((4, 256, 1024), BF),
                   jax.ShapeDtypeStruct((4, 1024, 256), F32)),
        in_specs=[pl.BlockSpec(memory_space=pltpu.VMEM),
                  pl.BlockSpec(memory_space=pltpu.VMEM)],
        out_specs=(pl.BlockSpec(memory_space=pl.ANY),
                   pl.BlockSpec(memory_space=pl.ANY)),
        scratch_shapes=[pltpu.VMEM((4, 1024, 256), F32), dma((8,))],
        compiler_params=pltpu.CompilerParams(vmem_limit_bytes=24 * 1024 * 1024),
        name="finish",
    )(gathered, partial)


def solution(mesh):
    in_specs = (P("blk", "rep", None), P("blk", None), P("blk", None))
    out_specs = (P("blk", "rep", None), P("blk", None, "rep"))
    return jax.shard_map(body, mesh=mesh, in_specs=in_specs, out_specs=out_specs, check_vma=False)
```
